32 devices in a mesh: dp: 4 (over z), fsdp: 4 (over x, core), tensor: 2 (over y).
Axes of the slice: x: 2, y: 2, z: 4, core: 2. Of those that a mesh axis runs over, the one named last changes fastest.
Arguments:
- tokens: bfloat16 [4096, 8192], P(('dp', 'fsdp'), 'tensor'), may hold values from -700 to 700
- queries: bfloat16 [4096, 8192], P(('dp', 'fsdp'), 'tensor'), may hold values from -140 to 140
- segment_ids: int32 [32, 128], P(('dp', 'fsdp')), may hold values from 0 to 3, never falling along the last dimension, each value on 1 to 64 neighbouring positions
- gain: float32 [8192], P('tensor'), may hold values from 0.1 to 1.9
- key_value_weight: bfloat16 [8192, 2048], P('tensor', 'fsdp'), may hold values from -0.0625 to 0.0625
- plan: int32 [8], replicated, may hold values from 0 to 7, as said below
Outputs:
- attended: bfloat16 [4096, 8192], P(('dp', 'fsdp'), 'tensor')
The draws below stay inside these ranges and needn't reach their ends.
Inputs may be any that keep to these rules, and one draw needn't show every extreme that they name: plan is a permutation of 0 to 7; from one dp index to another at most 1 micro-batches go, and in every draw some pair of dp indices carries exactly 1.
All inputs are finite; a program needn't handle non-finite values.
Results may differ from the reference program's by a relative error of at most 0.011.
Values may be sent and summed in bfloat16 or wider, within the bound.
A program may use at most 64 MiB of HBM per device.

```python
import math
import jax
import jax.numpy as jnp
import numpy as np
from jax import lax

MODEL_WIDTH = 8192
QUERY_HEADS = 64
KEY_VALUE_HEADS = 8
HEAD_SIZE = 128
MICRO_TOKENS = 128
MB_DEV = 2
CAP = 1
MICRO = 8
BATCHES = 32
TOKENS = 4096
N_DP = 4
N_FSDP = 4


def draw_tokens(key, part):
    keys = jax.random.split(key, 3)
    columns = jnp.arange(MODEL_WIDTH, dtype=jnp.float32) / MODEL_WIDTH
    base = jnp.clip(jax.random.normal(keys[0], (TOKENS, MODEL_WIDTH), jnp.float32), -4.0, 4.0)
    ramp = jnp.sqrt(1.0 + 2.0 * columns)
    row_scale = jnp.exp(jax.random.uniform(keys[1], (TOKENS, 1), minval=0.0, maxval=math.log(10.0)))
    column_scale = jnp.exp(jax.random.uniform(keys[2], (1, MODEL_WIDTH), minval=0.0, maxval=math.log(10.0))) * ramp[None, :]
    return (base * row_scale * column_scale).astype(jnp.bfloat16)


def draw_queries(key, part):
    keys = jax.random.split(key, 1)
    values = jnp.clip(jax.random.normal(keys[0], (TOKENS, QUERY_HEADS * HEAD_SIZE), jnp.float32), -4.0, 4.0)
    return values.astype(jnp.bfloat16)


def draw_plan(key, part):
    keys = jax.random.split(key, 4)
    offsets = jax.random.permutation(keys[0], N_DP)
    arrangement = jax.random.permutation(keys[1], MB_DEV)
    shifting = offsets[arrangement // CAP]
    target_slot = jax.random.permutation(keys[2], MB_DEV)
    relabel = jax.random.permutation(keys[3], N_DP)
    relabel_back = jnp.argsort(relabel)
    sources = jnp.arange(N_DP, dtype=jnp.int32)
    target_rank = relabel[(relabel_back[sources][:, None] + shifting[None, :]) % N_DP]
    layout = target_rank * MB_DEV + target_slot[None, :]
    return layout.reshape(MICRO).astype(jnp.int32)


def block_levels(own_key, dims, pieces, smallest, high):
    def one(position, parts):
        heights = jax.random.uniform(jax.random.fold_in(jax.random.fold_in(own_key, 6), position), (parts,), jnp.float32, smallest / len(pieces), high / len(pieces))
        return jnp.repeat(jnp.exp(heights), dims[position] // parts).reshape((-1,) + (1,) * (len(dims) - position - 1))

    level = one(*pieces[0])
    for cut in pieces[1:]:
        level = level * one(*cut)
    return level


def profile(number_of, total, bound, skew):
    weights = [(1 << 20) // math.isqrt(standing ** skew) + 1 for standing in range(2, number_of + 1)]
    rest, counts = total - bound - (number_of - 1), [1] * (number_of - 1)
    while rest > 0:
        movable = [i for i in range(number_of - 1) if counts[i] < bound]
        whole, left = sum([weights[i] for i in movable]), rest
        for i in movable:
            addition = min(bound - counts[i], max(1, left * weights[i] // whole), rest)
            counts[i] = counts[i] + addition
            rest = rest - addition
    return np.array([bound] + counts)


def ragged(rng, count, total, most, skew):
    if count == 2:
        one = jax.random.randint(rng, (), max(1, total - most), min(most, total - 1) + 1)
        return jnp.stack([one, total - one])
    lengths = jnp.asarray(profile(count, total, most, skew), jnp.int32)
    couples = (count - 1) // 2
    source_of, taker = lengths[1:1 + 2 * couples:2], lengths[2:2 + 2 * couples:2]
    margin = jnp.minimum(source_of - 1, most - taker)
    moved = jax.random.randint(jax.random.fold_in(rng, 1), (couples,), 0, 1 << 20) % (margin + 1)
    lengths = lengths.at[1:1 + 2 * couples:2].set(source_of - moved).at[2:2 + 2 * couples:2].set(taker + moved)
    return lengths[jax.random.permutation(jax.random.fold_in(rng, 2), count)]


def noise(rng, extent, spread, limit, pieces=(), held_as=jnp.bfloat16):
    loudness = block_levels(rng, extent, pieces, -0.22, 0.18) if pieces else 1.0
    values = jax.random.normal(rng, extent, jnp.float32) * spread * loudness
    return jnp.minimum(jnp.maximum(values, -limit), limit).astype(held_as)


def setup_inputs(seed: int = 0) -> dict:
    key_of = jax.random.split(jax.random.key(seed), 7)
    tokens = draw_tokens(jax.random.fold_in(key_of[6], 71), 0)
    queries = draw_queries(jax.random.fold_in(key_of[6], 71), 0)
    segment_ids = jax.vmap(lambda own: jnp.searchsorted(jnp.cumsum(ragged(own, 4, MICRO_TOKENS, MICRO_TOKENS // 2, 1)), jnp.arange(MICRO_TOKENS), side="right"))(jax.random.split(key_of[2], BATCHES)).reshape((BATCHES, MICRO_TOKENS)).astype(jnp.int32)
    gain = jnp.clip(1.0 + 0.18 * jax.random.normal(key_of[3], (MODEL_WIDTH,), jnp.float32), 0.1, 1.9)
    key_value_weight = noise(key_of[4], (MODEL_WIDTH, 2 * KEY_VALUE_HEADS * HEAD_SIZE), MODEL_WIDTH ** -0.5, 0.0625, ((0, 2), (1, 4)))
    plan = draw_plan(jax.random.fold_in(key_of[6], 71), 0)
    return dict(tokens=tokens, queries=queries, segment_ids=segment_ids, gain=gain, key_value_weight=key_value_weight, plan=plan)


epsilon = 1e-05

def attend_block(query_block, key_block, value_block, doc_block):
    scores = jnp.einsum('qhgd,khd->hgqk', query_block, key_block, precision=lax.Precision.HIGHEST) * HEAD_SIZE ** (-0.5)
    positions = jnp.arange(MICRO_TOKENS, dtype=jnp.int32)
    allowed = (doc_block[:, None] == doc_block[None, :]) & (positions[:, None] >= positions[None, :])
    scores = jnp.where(allowed[None, None], scores, -1e+30)
    row_max = lax.optimization_barrier(jnp.max(scores, axis=-1, keepdims=True))
    expo = jnp.exp(scores - row_max)
    weights = (expo / lax.optimization_barrier(jnp.sum(expo, axis=-1, keepdims=True))).astype(jnp.bfloat16)
    mixed = jnp.einsum('hgqk,khd->qhgd', weights.astype(jnp.float32), value_block, precision=lax.Precision.HIGHEST)
    return mixed.reshape(MICRO_TOKENS, QUERY_HEADS * HEAD_SIZE).astype(jnp.bfloat16)

def reference(tokens, queries, segment_ids, gain, key_value_weight, plan):
    complete_weight = key_value_weight.astype(jnp.float32)
    head_group = QUERY_HEADS // KEY_VALUE_HEADS

    def one_block(item):
        rows, query_row_block, doc_row = item
        values = rows.astype(jnp.float32)
        scale = lax.rsqrt(lax.optimization_barrier(jnp.sum(values * values, axis=1)) / MODEL_WIDTH + epsilon)
        normed = (values * scale[:, None] * gain).astype(jnp.bfloat16)
        key_value_rows = jnp.dot(normed.astype(jnp.float32), complete_weight, precision=lax.Precision.HIGHEST)
        key_value_heads = key_value_rows.reshape(MICRO_TOKENS, KEY_VALUE_HEADS, 2, HEAD_SIZE)
        query_head_count = query_row_block.astype(jnp.float32).reshape(MICRO_TOKENS, KEY_VALUE_HEADS, head_group, HEAD_SIZE)
        return attend_block(query_head_count, key_value_heads[:, :, 0], key_value_heads[:, :, 1], doc_row)
    blocks = lax.map(one_block, (tokens.reshape(BATCHES, MICRO_TOKENS, MODEL_WIDTH), queries.reshape(BATCHES, MICRO_TOKENS, QUERY_HEADS * HEAD_SIZE), segment_ids))
    grid = blocks.reshape(N_DP, N_FSDP, MB_DEV, MICRO_TOKENS, QUERY_HEADS * HEAD_SIZE).transpose(1, 0, 2, 3, 4).reshape(N_FSDP, MICRO, MICRO_TOKENS, QUERY_HEADS * HEAD_SIZE)
    inverse = jnp.argsort(plan).astype(jnp.int32)
    moved = grid[:, inverse]
    return moved.reshape(N_FSDP, N_DP, MB_DEV, MICRO_TOKENS, QUERY_HEADS * HEAD_SIZE).transpose(1, 0, 2, 3, 4).reshape(TOKENS, QUERY_HEADS * HEAD_SIZE)
```

```python
import functools

import jax
import jax.numpy as jnp
from jax import lax
from jax.experimental import pallas as pl
from jax.experimental.pallas import tpu as pltpu
from jax.sharding import PartitionSpec as P

HEAD_SIZE = 128


epsilon = 1e-05


def pack_query_kernel(send_ref, query_ref, out_ref):
    out_ref[...] = query_ref[...]


def pack_queries(send_index, queries, length):
    ranks = send_index.shape[0]
    width = queries.shape[1]
    return pl.pallas_call(
        pack_query_kernel,
        grid_spec=pltpu.PrefetchScalarGridSpec(
            num_scalar_prefetch=1,
            grid=(ranks,),
            in_specs=[pl.BlockSpec((length, width), lambda r, send: (send[r], 0))],
            out_specs=pl.BlockSpec((length, width), lambda r, send: (r, 0)),
        ),
        out_shape=jax.ShapeDtypeStruct((ranks * length, width), queries.dtype),
        name="pack_queries",
    )(send_index, queries)


def pack_kv_kernel(heads_kv, send_ref, kv_ref, document_ref, out_ref):
    for h in range(heads_kv):
        key = kv_ref[:, 2 * h * HEAD_SIZE : (2 * h + 1) * HEAD_SIZE]
        high = key.astype(jnp.bfloat16)
        low = (key - high.astype(jnp.float32)).astype(jnp.bfloat16)
        value = kv_ref[:, (2 * h + 1) * HEAD_SIZE : (2 * h + 2) * HEAD_SIZE]
        for place, part in enumerate((high, low, value.astype(jnp.bfloat16))):
            start = (place * heads_kv + h) * HEAD_SIZE
            out_ref[:, start : start + HEAD_SIZE] = part
    out_ref[:, 3 * heads_kv * HEAD_SIZE :] = document_ref[...]


def pack_kv(send_index, kv, documents, length):
    ranks = send_index.shape[0]
    width = kv.shape[1]
    heads_kv = width // (2 * HEAD_SIZE)
    packed = (3 * heads_kv + 1) * HEAD_SIZE
    return pl.pallas_call(
        functools.partial(pack_kv_kernel, heads_kv),
        grid_spec=pltpu.PrefetchScalarGridSpec(
            num_scalar_prefetch=1,
            grid=(ranks,),
            in_specs=[
                pl.BlockSpec((length, width), lambda r, send: (send[r], 0)),
                pl.BlockSpec((length, HEAD_SIZE), lambda r, send: (send[r], 0)),
            ],
            out_specs=pl.BlockSpec((length, packed), lambda r, send: (r, 0)),
        ),
        out_shape=jax.ShapeDtypeStruct((ranks * length, packed), jnp.bfloat16),
        name="pack_kv",
    )(send_index, kv, documents)


def attend_kernel(
    head_group, keep_ref, query_ref, high_ref, low_ref, value_ref, document_ref, out_ref
):
    length = query_ref.shape[0]
    query = jnp.concatenate(
        [query_ref[:, g * HEAD_SIZE : (g + 1) * HEAD_SIZE] for g in range(head_group)], axis=0
    )
    across = (((1,), (1,)), ((), ()))
    scores = lax.dot_general(query, high_ref[...], across, preferred_element_type=jnp.float32)
    scores += lax.dot_general(query, low_ref[...], across, preferred_element_type=jnp.float32)
    scores = (scores * HEAD_SIZE ** (-0.5)).reshape(head_group, length, length)
    document = document_ref[...].astype(jnp.float32)
    rows = lax.broadcasted_iota(jnp.int32, (length, length), 0)
    columns = lax.broadcasted_iota(jnp.int32, (length, length), 1)
    allowed = (document == document.T) & (columns <= rows)
    scores = jnp.where(allowed[None], scores, -1e30)
    row_max = jnp.max(scores, axis=-1, keepdims=True)
    expo = jnp.exp(scores - row_max)
    weights = (expo / jnp.sum(expo, axis=-1, keepdims=True)).astype(jnp.bfloat16)
    mixed = jnp.dot(
        weights.reshape(head_group * length, length),
        value_ref[...],
        preferred_element_type=jnp.float32,
    ).astype(jnp.bfloat16)
    for g in range(head_group):
        out_ref[:, g * HEAD_SIZE : (g + 1) * HEAD_SIZE] = mixed[g * length : (g + 1) * length]


def attend(keep_index, queries, packed, length):
    batches = keep_index.shape[0]
    heads_kv = (packed.shape[1] // HEAD_SIZE - 1) // 3
    width = queries.shape[1]
    group_width = width // heads_kv

    def part(place):
        return pl.BlockSpec(
            (length, HEAD_SIZE), lambda s, h, keep: (keep[s], place * heads_kv + h)
        )

    return pl.pallas_call(
        functools.partial(attend_kernel, group_width // HEAD_SIZE),
        grid_spec=pltpu.PrefetchScalarGridSpec(
            num_scalar_prefetch=1,
            grid=(batches, heads_kv),
            in_specs=[
                pl.BlockSpec((length, group_width), lambda s, h, keep: (keep[s], h)),
                part(0),
                part(1),
                part(2),
                pl.BlockSpec((length, HEAD_SIZE), lambda s, h, keep: (keep[s], 3 * heads_kv)),
            ],
            out_specs=pl.BlockSpec((length, group_width), lambda s, h, keep: (s, h)),
        ),
        out_shape=jax.ShapeDtypeStruct((batches * length, width), jnp.bfloat16),
        name="attend",
    )(keep_index, queries, packed, packed, packed, packed)


def project(rows, gain, key_value_weight):
    values = rows.astype(jnp.float32)
    stats = lax.psum(jnp.sum(values * values, axis=1), "tensor")
    full_width = rows.shape[1] * lax.axis_size("tensor")
    scale = lax.rsqrt(stats / full_width + epsilon)
    normed = (values * scale[:, None] * gain).astype(jnp.bfloat16)
    partial_value = jnp.dot(
        normed,
        lax.all_gather(key_value_weight, "fsdp", axis=1, tiled=True),
        preferred_element_type=jnp.float32,
    )
    return lax.psum_scatter(partial_value, "tensor", scatter_dimension=1, tiled=True)


def shards(tokens, queries, segment_ids, gain, key_value_weight, plan):
    rank_count = lax.axis_size("dp")
    own_rank = lax.axis_index("dp")
    batches, length = segment_ids.shape
    own_dest = lax.dynamic_slice_in_dim(plan, own_rank * batches, batches) // batches
    rank_range = jnp.arange(rank_count, dtype=jnp.int32)
    slot_range = jnp.arange(batches, dtype=jnp.int32)
    send_index = jnp.sum(
        jnp.where(own_dest[None, :] == rank_range[:, None], slot_range[None, :], 0), axis=1
    )
    position = jnp.arange(plan.shape[0], dtype=jnp.int32)
    own_slots = own_rank * batches + slot_range
    keep_index = jnp.sum(
        jnp.where(plan[None, :] == own_slots[:, None], position[None, :] // batches, 0), axis=1
    )
    moved_queries = lax.all_to_all(
        pack_queries(send_index, queries, length), "dp", split_axis=0, concat_axis=0, tiled=True
    )
    documents = jnp.broadcast_to(
        segment_ids.reshape(batches * length, 1).astype(jnp.bfloat16),
        (batches * length, HEAD_SIZE),
    )
    kv = project(tokens, gain, key_value_weight)
    moved_kv = lax.all_to_all(
        pack_kv(send_index, kv, documents, length), "dp", split_axis=0, concat_axis=0, tiled=True
    )
    return attend(keep_index, moved_queries, moved_kv, length)


def solution(mesh):
    placed = (
        P(("dp", "fsdp"), "tensor"),
        P(("dp", "fsdp"), "tensor"),
        P(("dp", "fsdp"), None),
        P("tensor"),
        P("tensor", "fsdp"),
        P(),
    )
    return jax.shard_map(
        shards, mesh=mesh, in_specs=placed, out_specs=P(("dp", "fsdp"), "tensor"), check_vma=False
    )
```

```python
import functools

import jax
import jax.numpy as jnp
from jax import lax
from jax.experimental import pallas as pl
from jax.experimental.pallas import tpu as pltpu
from jax.sharding import PartitionSpec as P


HEAD_SIZE = 128


epsilon = 1e-05


def pack_query_kernel(send_ref, query_ref, out_ref):
    out_ref[...] = query_ref[...]


def pack_queries(send_index, queries, length):
    ranks = send_index.shape[0]
    width = queries.shape[1]
    return pl.pallas_call(
        pack_query_kernel,
        grid_spec=pltpu.PrefetchScalarGridSpec(
            num_scalar_prefetch=1,
            grid=(ranks,),
            in_specs=[pl.BlockSpec((length, width), lambda r, send: (send[r], 0))],
            out_specs=pl.BlockSpec((length, width), lambda r, send: (r, 0)),
        ),
        out_shape=jax.ShapeDtypeStruct((ranks * length, width), queries.dtype),
        name="pack_queries",
    )(send_index, queries)


def split_partial_kernel(part_ref, out_ref):
    key = part_ref[:, :HEAD_SIZE]
    high = key.astype(jnp.bfloat16)
    out_ref[:, :HEAD_SIZE] = high
    out_ref[:, HEAD_SIZE : 2 * HEAD_SIZE] = (key - high.astype(jnp.float32)).astype(jnp.bfloat16)
    out_ref[:, 2 * HEAD_SIZE :] = part_ref[:, HEAD_SIZE:].astype(jnp.bfloat16)


def split_partial(partial_value, ranks, spread):
    rows, width = partial_value.shape
    all_heads = width // (2 * HEAD_SIZE)
    heads = all_heads // spread
    height = rows // ranks
    return pl.pallas_call(
        split_partial_kernel,
        grid=(spread, ranks, heads),
        in_specs=[pl.BlockSpec((height, 2 * HEAD_SIZE), lambda b, f, h: (f, b * heads + h))],
        out_specs=pl.BlockSpec(
            (height, 3 * HEAD_SIZE), lambda b, f, h: ((b * ranks + f) * heads + h, 0)
        ),
        out_shape=jax.ShapeDtypeStruct((ranks * all_heads * height, 3 * HEAD_SIZE), jnp.bfloat16),
        name="split_partial",
    )(partial_value)


def pack_kv_kernel(sources, send_ref, slot_ref, *refs):
    *part_refs, document_ref, out_ref = refs
    part_heads = part_refs[0].shape[1]
    heads_kv = part_heads * len(part_refs) // sources
    for h in range(heads_kv):
        first = h // part_heads * sources
        key = value = 0.0
        for part_ref in part_refs[first : first + sources]:
            block = part_ref[0, h % part_heads, 0].astype(jnp.float32)
            key += block[:, :HEAD_SIZE] + block[:, HEAD_SIZE : 2 * HEAD_SIZE]
            value += block[:, 2 * HEAD_SIZE :]
        high = key.astype(jnp.bfloat16)
        low = (key - high.astype(jnp.float32)).astype(jnp.bfloat16)
        for place, part in enumerate((high, low, value.astype(jnp.bfloat16))):
            start = (place * heads_kv + h) * HEAD_SIZE
            out_ref[:, start : start + HEAD_SIZE] = part
    out_ref[:, 3 * heads_kv * HEAD_SIZE :] = document_ref[...]


def pack_kv(send_index, slot_index, parts, documents, sources, length):
    ranks = send_index.shape[0]
    count = slot_index.shape[0]
    rows = documents.shape[0]
    part_heads = parts.shape[0] // (count * rows)
    packed = (3 * part_heads * count // sources + 1) * HEAD_SIZE

    def arrived(w):
        return pl.BlockSpec(
            (1, part_heads, 1, length, 3 * HEAD_SIZE),
            lambda r, send, slot: (slot[w], 0, send[r], 0, 0),
        )

    view = parts.reshape(count, part_heads, rows // length, length, 3 * HEAD_SIZE)
    return pl.pallas_call(
        functools.partial(pack_kv_kernel, sources),
        grid_spec=pltpu.PrefetchScalarGridSpec(
            num_scalar_prefetch=2,
            grid=(ranks,),
            in_specs=[arrived(w) for w in range(count)]
            + [pl.BlockSpec((length, HEAD_SIZE), lambda r, send, slot: (send[r], 0))],
            out_specs=pl.BlockSpec((length, packed), lambda r, send, slot: (r, 0)),
        ),
        out_shape=jax.ShapeDtypeStruct((ranks * length, packed), jnp.bfloat16),
        name="pack_kv",
    )(send_index, slot_index, *[view] * count, documents)


def attend_kernel(
    head_group, keep_ref, query_ref, high_ref, low_ref, value_ref, document_ref, out_ref
):
    length = query_ref.shape[0]
    query = jnp.concatenate(
        [query_ref[:, g * HEAD_SIZE : (g + 1) * HEAD_SIZE] for g in range(head_group)], axis=0
    )
    across = (((1,), (1,)), ((), ()))
    scores = lax.dot_general(query, high_ref[...], across, preferred_element_type=jnp.float32)
    scores += lax.dot_general(query, low_ref[...], across, preferred_element_type=jnp.float32)
    scores = (scores * HEAD_SIZE ** (-0.5)).reshape(head_group, length, length)
    document = document_ref[...].astype(jnp.float32)
    rows = lax.broadcasted_iota(jnp.int32, (length, length), 0)
    columns = lax.broadcasted_iota(jnp.int32, (length, length), 1)
    allowed = (document == document.T) & (columns <= rows)
    scores = jnp.where(allowed[None], scores, -1e30)
    row_max = jnp.max(scores, axis=-1, keepdims=True)
    expo = jnp.exp(scores - row_max)
    weights = (expo / jnp.sum(expo, axis=-1, keepdims=True)).astype(jnp.bfloat16)
    mixed = jnp.dot(
        weights.reshape(head_group * length, length),
        value_ref[...],
        preferred_element_type=jnp.float32,
    ).astype(jnp.bfloat16)
    for g in range(head_group):
        out_ref[:, g * HEAD_SIZE : (g + 1) * HEAD_SIZE] = mixed[g * length : (g + 1) * length]


def attend(keep_index, queries, packed, length):
    batches = keep_index.shape[0]
    heads_kv = (packed.shape[1] // HEAD_SIZE - 1) // 3
    width = queries.shape[1]
    group_width = width // heads_kv

    def part(place):
        return pl.BlockSpec(
            (length, HEAD_SIZE), lambda s, h, keep: (keep[s], place * heads_kv + h)
        )

    return pl.pallas_call(
        functools.partial(attend_kernel, group_width // HEAD_SIZE),
        grid_spec=pltpu.PrefetchScalarGridSpec(
            num_scalar_prefetch=1,
            grid=(batches, heads_kv),
            in_specs=[
                pl.BlockSpec((length, group_width), lambda s, h, keep: (keep[s], h)),
                part(0),
                part(1),
                part(2),
                pl.BlockSpec((length, HEAD_SIZE), lambda s, h, keep: (keep[s], 3 * heads_kv)),
            ],
            out_specs=pl.BlockSpec((length, group_width), lambda s, h, keep: (s, h)),
        ),
        out_shape=jax.ShapeDtypeStruct((batches * length, width), jnp.bfloat16),
        name="attend",
    )(keep_index, queries, packed, packed, packed, packed)


def project(rows, gain, key_value_weight):
    all_rows = lax.all_gather(rows, "fsdp", axis=0, tiled=True)
    values = rows.astype(jnp.float32)
    own_stats = jnp.sum(values * values, axis=1)
    stats = lax.psum(own_stats, "tensor")
    full_width = rows.shape[1] * lax.axis_size("tensor")
    scale = lax.all_gather(lax.rsqrt(stats / full_width + epsilon), "fsdp", axis=0, tiled=True)
    normed = (all_rows.astype(jnp.float32) * scale[:, None] * gain).astype(jnp.bfloat16)
    partial_value = jnp.dot(normed, key_value_weight, preferred_element_type=jnp.float32)
    f_ranks, t_ranks = lax.axis_size("fsdp"), lax.axis_size("tensor")
    joined, spread = max(1, f_ranks // t_ranks), max(1, t_ranks // f_ranks)
    count = f_ranks * spread
    parts = split_partial(partial_value, f_ranks, spread)
    share = parts.shape[0] // count
    f, t = lax.axis_index("fsdp"), lax.axis_index("tensor")
    number = f % joined * t_ranks + t
    arrived = []
    for p in range(count):
        pairs = []
        for i in range(f_ranks):
            for j in range(t_ranks):
                block = (i % joined * t_ranks + j + p) % count
                target = i // joined * spread + block // f_ranks
                pairs.append((i * t_ranks + j, block % f_ranks * t_ranks + target))
        sent = lax.dynamic_slice_in_dim(parts, (number + p) % count * share, share)
        arrived.append(lax.ppermute(sent, ("fsdp", "tensor"), pairs))
    slot_index = (t % spread * f_ranks + f - jnp.arange(count, dtype=jnp.int32)) % count
    return jnp.concatenate(arrived), slot_index


def shards(tokens, queries, segment_ids, gain, key_value_weight, plan):
    rank_count = lax.axis_size("dp")
    own_rank = lax.axis_index("dp")
    batches, length = segment_ids.shape
    own_dest = lax.dynamic_slice_in_dim(plan, own_rank * batches, batches) // batches
    rank_range = jnp.arange(rank_count, dtype=jnp.int32)
    slot_range = jnp.arange(batches, dtype=jnp.int32)
    send_index = jnp.sum(
        jnp.where(own_dest[None, :] == rank_range[:, None], slot_range[None, :], 0), axis=1
    )
    position = jnp.arange(plan.shape[0], dtype=jnp.int32)
    own_slots = own_rank * batches + slot_range
    keep_index = jnp.sum(
        jnp.where(plan[None, :] == own_slots[:, None], position[None, :] // batches, 0), axis=1
    )
    parcels = pack_queries(send_index, queries, length)
    moved_queries = lax.all_to_all(parcels, "dp", split_axis=0, concat_axis=0, tiled=True)
    documents = jnp.broadcast_to(
        segment_ids.reshape(batches * length, 1).astype(jnp.bfloat16),
        (batches * length, HEAD_SIZE),
    )
    parts, slot_index = project(tokens, gain, key_value_weight)
    packed = pack_kv(
        send_index, slot_index, parts, documents, lax.axis_size("tensor"), length
    )
    packed, moved_queries = lax.optimization_barrier((packed, moved_queries))
    moved_kv = lax.all_to_all(packed, "dp", split_axis=0, concat_axis=0, tiled=True)
    return attend(keep_index, moved_queries, moved_kv, length)


def solution(mesh):
    placed = (
        P(("dp", "fsdp"), "tensor"),
        P(("dp", "fsdp"), "tensor"),
        P(("dp", "fsdp"), None),
        P("tensor"),
        P("tensor", "fsdp"),
        P(),
    )
    return jax.shard_map(
        shards, mesh=mesh, in_specs=placed, out_specs=P(("dp", "fsdp"), "tensor"), check_vma=False
    )
```
